256 devices in a mesh: trial: 4 (over z_lo), south: 4 (over y_lo, core), east: 4 (over x), down: 4 (over z_hi, y_hi).
Axes of the slice: x: 4, y: 4 (y_hi: 2, y_lo: 2; y = y_hi * 2 + y_lo), z: 8 (z_hi: 2, z_lo: 4; z = z_hi * 4 + z_lo), core: 2. Of those that a mesh axis runs over, the one named last changes fastest.
Arguments:
- tracer: float32 [64, 64, 512, 128], P(('trial', 'south'), 'east', 'down'), parts along dimension 0, may hold values from 0.5 to 2
- mobility: float32 [64, 64, 512, 128], P(('trial', 'south'), 'east', 'down'), parts along dimension 0, may hold values from 0.03 to 0.15
- source: float32 [64, 64, 512, 128], P(('trial', 'south'), 'east', 'down'), parts along dimension 0, may hold values from -0.2 to 0.2
Outputs:
- standardized: float32 [64, 64, 512, 128], P(('trial', 'south'), 'east', 'down'), parts along dimension 0
- tracer_end: float32 [64, 64, 512, 128], P(('trial', 'south'), 'east', 'down'), parts along dimension 0
The draws below stay inside these ranges and needn't reach their ends.
There are 4 independent parts, one for each index of `trial`. The reference program is written for one: setup_inputs(seed, part) draws one part's arguments, and reference() takes and returns one part's arrays. A program takes and returns all parts, laid end to end along the dimension named above; each array names one. Nothing has to cross between parts.
All inputs are finite; a program needn't handle non-finite values.
Results may differ from the reference program's by a relative error of at most 0.00002.
Values sent between devices are 32-bit elements; how exact they have to be, the bound alone decides.
No kernel may reach another device: no remote copies, remote signals or barrier semaphores. Data moves between devices by JAX's collectives and lax.ppermute only.
A program may use at most 128 MiB of HBM per device.

```python
import jax
import jax.numpy as jnp
from jax import lax

GRID_Y = 16
GRID_X = 64
GRID_Z = 512
LEVELS = 128
STEPS = 3


def level_of(stream_key, shape, split, least, top_value):
    level = 1.0
    for axis_at, shards_of in split:
        heights = jax.random.uniform(jax.random.fold_in(jax.random.fold_in(stream_key, 6), axis_at), (shards_of,), jnp.float32, least / len(split), top_value / len(split))
        level = level * jnp.repeat(jnp.exp(heights), shape[axis_at] // shards_of).reshape((-1,) + (1,) * (len(shape) - 1 - axis_at))
    return level


def setup_inputs(seed: int = 0, part: int = 0) -> dict:
    arg_keys = jax.random.split(jax.random.key(seed), 4)
    part_keys = jax.random.split(jax.random.fold_in(arg_keys[3], part), 4)
    tracer = jnp.clip(0.5 + 1.5 * jax.random.uniform(part_keys[0], (GRID_Y, GRID_X, GRID_Z, LEVELS), jnp.float32) ** level_of(part_keys[0], (GRID_Y, GRID_X, GRID_Z, LEVELS), ((0, 4), (1, 4), (2, 4)), -0.2, 0.2), 0.5, 2.0)
    mobility = jnp.clip(0.03 + 0.120000007 * jax.random.uniform(part_keys[1], (GRID_Y, GRID_X, GRID_Z, LEVELS), jnp.float32) ** level_of(part_keys[1], (GRID_Y, GRID_X, GRID_Z, LEVELS), ((0, 4), (1, 4), (2, 4)), -0.2, 0.2), 0.03, 0.15)
    source = jnp.clip(jax.random.uniform(part_keys[2], (GRID_Y, GRID_X, GRID_Z, LEVELS), jnp.float32, -0.2, 0.2) * level_of(part_keys[2], (GRID_Y, GRID_X, GRID_Z, LEVELS), ((0, 4), (1, 4), (2, 4)), -0.4, 0.0), -0.2, 0.2)
    return dict(tracer=tracer, mobility=mobility, source=source)


def strip_edges(values, dims):
    for dim in dims:
        values = lax.slice_in_dim(values, 1, values.shape[dim] - 1, axis=dim)
    return values

def neighbour(values, dim, start, dims):
    others = [other for other in dims if other != dim]
    values = strip_edges(values, others)
    return lax.slice_in_dim(values, start, start + values.shape[dim] - 2, axis=dim)

def one_step(padded, mobility, source):
    middle = strip_edges(padded, (0, 1, 2))
    lower = [neighbour(padded, dim, 0, (0, 1, 2)) for dim in (0, 1, 2)]
    upper = [neighbour(padded, dim, 2, (0, 1, 2)) for dim in (0, 1, 2)]
    spread = lower[0] + upper[0] + lower[1] + upper[1] + lower[2] + upper[2] - 6.0 * middle
    return middle + mobility * spread + source

def reference(tracer, mobility, source):
    for step in range(STEPS):
        tracer = one_step(jnp.pad(tracer, ((1, 1), (1, 1), (1, 1), (0, 0)), mode='wrap'), mobility, source)
    line_mean = lax.optimization_barrier(jnp.mean(tracer, axis=2, keepdims=True))
    centred = tracer - line_mean
    line_variance = lax.optimization_barrier(jnp.mean(centred * centred, axis=2, keepdims=True))
    standardized = centred * lax.rsqrt(line_variance + 0.0001)
    return (standardized, tracer)
```

```python
import functools

import jax
import jax.numpy as jnp
from jax import lax
from jax.experimental import pallas as pl
from jax.experimental.pallas import tpu as pltpu
from jax.sharding import PartitionSpec as P

STEPS = 3
VMEM_LIMIT = 16 * 1024 * 1024
PARAMS = pltpu.CompilerParams(vmem_limit_bytes=VMEM_LIMIT)


def f32(*shape):
    return jax.ShapeDtypeStruct(shape, jnp.float32)


def rows_of(refs):
    if len(refs) == 1:
        return [refs[0].at[r] for r in range(refs[0].shape[0])]
    first, middle, last = refs
    return [first] + [middle.at[r] for r in range(middle.shape[0])] + [last]


def partial_kernel(n, *refs):
    tracer = rows_of(refs[:n])
    mobility, source, low_x, high_x = refs[n : n + 4]
    out = rows_of(refs[n + 4 :])
    width, depth, _ = tracer[0].shape
    z = lax.broadcasted_iota(jnp.int32, tracer[0].shape[1:], 0)

    def cell(r, x, before, after):
        here = tracer[r][x]
        spread = before + after
        if r > 0:
            spread += tracer[r - 1][x]
        if r < len(tracer) - 1:
            spread += tracer[r + 1][x]
        spread += jnp.where(z == 0, 0.0, pltpu.roll(here, 1, 0))
        spread += jnp.where(z == depth - 1, 0.0, pltpu.roll(here, depth - 1, 0))
        out[r][x] = here + mobility[r, x] * (spread - 6.0 * here) + source[r, x]

    for r in range(len(tracer)):
        cell(r, 0, low_x[r], tracer[r][1])

        @pl.loop(1, width - 1)
        def _(x, r=r):
            cell(r, x, tracer[r][x - 1], tracer[r][x + 1])

        cell(r, width - 1, tracer[r][width - 2], high_x[r])


def add_lines(row, mobility, low_z, high_z, r, x):
    depth = row.shape[1]
    row[x, 0:1] += mobility[r, x, 0:1] * low_z[r, pl.ds(x, 1)]
    row[x, depth - 1 : depth] += mobility[r, x, depth - 1 : depth] * high_z[r, pl.ds(x, 1)]


def finish_kernel(first_in, middle_in, last_in, mobility, low_y, high_y, low_z, high_z, first, middle, last, *edges):
    first_x, last_x, first_z, last_z = edges
    width, depth, _ = first.shape
    rows = rows_of((first, middle, last))
    top = len(rows) - 1

    @pl.loop(0, width)
    def _(x):
        first[x] = first_in[x] + mobility[0, x] * low_y[x]
        last[x] = last_in[x] + mobility[top, x] * high_y[x]

    for r, row in enumerate(rows):

        @pl.loop(0, width)
        def _(x, r=r, row=row):
            add_lines(row, mobility, low_z, high_z, r, x)
            first_z[r, pl.ds(x, 1)] = row[x, 0:1]
            last_z[r, pl.ds(x, 1)] = row[x, depth - 1 : depth]

        first_x[r] = row[0]
        last_x[r] = row[width - 1]


def last_kernel(first_in, middle_in, last_in, mobility, low_y, high_y, low_z, high_z, tracer, means, spreads):
    rows_in = rows_of((first_in, middle_in, last_in))
    top = len(rows_in) - 1
    width, depth, _ = first_in.shape
    z = lax.broadcasted_iota(jnp.int32, (depth, first_in.shape[2]), 0)

    for r, row in enumerate(rows_in):

        @pl.loop(0, width)
        def _(x, r=r, row=row):
            value = row[x]
            if r == 0:
                value += mobility[r, x] * low_y[x]
            if r == top:
                value += mobility[r, x] * high_y[x]
            lines = jnp.where(z == 0, low_z[r, pl.ds(x, 1)], 0.0)
            lines += jnp.where(z == depth - 1, high_z[r, pl.ds(x, 1)], 0.0)
            value += mobility[r, x] * lines
            tracer[r, x] = value
            mean = jnp.sum(value, axis=0, keepdims=True) * (1.0 / depth)
            off = value - mean
            means[r, pl.ds(x, 1)] = mean
            spreads[r, pl.ds(x, 1)] = jnp.sum(off * off, axis=0, keepdims=True)


def store_kernel(tracer, out, sem):
    copy = pltpu.make_async_copy(tracer, out, sem)
    copy.start()
    copy.wait()


def scale_kernel(tracer, *refs):
    *parts, out, held, sems = refs
    means, spreads = (parts[0::2], parts[1::2])
    count, width, depth, _ = tracer.shape
    copies = []
    for r in range(count):
        mean = sum(part[r] for part in means) * (1.0 / len(means))
        away = sum((part[r] - mean) * (part[r] - mean) for part in means)
        total = sum(part[r] for part in spreads) + depth * away
        scale = lax.rsqrt(total * (1.0 / (depth * len(means))) + 0.0001)
        for x in range(width):
            held[r, x] = (tracer[r, x] - mean[x : x + 1]) * scale[x : x + 1]
        copies.append(pltpu.make_async_copy(held.at[r], out.at[r], sems.at[r]))
        copies[-1].start()
    for copy in copies:
        copy.wait()


def body(tracer, mobility, source):
    count, width, depth, levels = tracer.shape
    row, middle = (f32(width, depth, levels), f32(count - 2, width, depth, levels))
    plane, line = (f32(count, depth, levels), f32(count, width, levels))

    def swap(leading, last, axis):
        peers = lax.axis_size(axis)
        up = [(i, (i + 1) % peers) for i in range(peers)]
        low = lax.ppermute(last, axis, up)
        high = lax.ppermute(leading, axis, [(b, a) for a, b in up])
        return (low, high)

    rows = (tracer,)
    ends = (tracer[0], tracer[-1])
    edges = (tracer[:, 0], tracer[:, -1], tracer[:, :, 0], tracer[:, :, -1])
    for step in range(STEPS):
        along_y = swap(*ends, "south")
        along_x = swap(*edges[:2], "east")
        along_z = swap(*edges[2:], "down")
        partial = pl.pallas_call(
            functools.partial(partial_kernel, len(rows)),
            out_shape=(row, middle, row),
            compiler_params=PARAMS,
            name="partial",
        )(*rows, mobility, source, *along_x)
        inputs = (*partial, mobility, *along_y, *along_z)
        if step < STEPS - 1:
            first, inner, last, *edges = pl.pallas_call(
                finish_kernel,
                out_shape=(row, middle, row, plane, plane, line, line),
                input_output_aliases={1: 1},
                compiler_params=PARAMS,
                name="finish",
            )(*inputs)
            rows = (first, inner, last)
            ends = (first, last)
    end, mean, spread = pl.pallas_call(
        last_kernel,
        out_shape=(f32(count, width, depth, levels), line, line),
        compiler_params=PARAMS,
        name="last",
    )(*inputs)
    peers = lax.axis_size("down")
    sums = jnp.stack([mean, spread])
    parts = [mean, spread]
    for away in range(peers - 1, 0, -1):
        other = lax.ppermute(sums, "down", [(i, i ^ away) for i in range(peers)])
        parts += [other[0], other[1]]
    stored = pl.pallas_call(
        store_kernel,
        out_shape=f32(count, width, depth, levels),
        out_specs=pl.BlockSpec(memory_space=pl.ANY),
        scratch_shapes=[pltpu.SemaphoreType.DMA],
        compiler_params=PARAMS,
        name="store",
    )(end)
    standardized = pl.pallas_call(
        scale_kernel,
        out_shape=f32(count, width, depth, levels),
        out_specs=pl.BlockSpec(memory_space=pl.ANY),
        scratch_shapes=[pltpu.VMEM((count, width, depth, levels), jnp.float32), pltpu.SemaphoreType.DMA((count,))],
        compiler_params=PARAMS,
        name="scale",
    )(end, *parts)
    return (standardized, stored)


def solution(mesh):
    spec = P(("trial", "south"), "east", "down", None)
    return jax.shard_map(body, mesh=mesh, in_specs=(spec,) * 3, out_specs=(spec,) * 2, check_vma=False)
```

```python
import functools

import jax
import jax.numpy as jnp
from jax import lax
from jax.experimental import pallas as pl
from jax.experimental.pallas import tpu as pltpu
from jax.sharding import PartitionSpec as P


STEPS = 3
RIM = 16


def f32(*shape):
    return jax.ShapeDtypeStruct(shape, jnp.float32)


def plane_of(pieces, x):
    if len(pieces) == 1:
        return pieces[0][x]
    inner, outer = pieces
    rim = outer.shape[1] // 2
    return jnp.concatenate([outer[x, :rim], inner[x], outer[x, rim:]], axis=0)


def rows_of(refs):
    if len(refs) == 1:
        return [(refs[0].at[r],) for r in range(refs[0].shape[0])]
    half = len(refs) // 2
    middle = refs[half]
    return [refs[:half]] + [(middle.at[r],) for r in range(middle.shape[0])] + [refs[half + 1 :]]


def line_stats(value):
    mean = jnp.sum(value, axis=0, keepdims=True) * (1.0 / value.shape[0])
    off = value - mean
    return mean, jnp.sum(off * off, axis=0, keepdims=True)


def partial_kernel(n, with_stats, *refs):
    tracer = rows_of(refs[:n])
    mobility, source, low_x, high_x, first, middle, last, *stats = refs[n:]
    top, width, depth, levels = (mobility.shape[0] - 1, *mobility.shape[1:])
    out = [first] + [middle.at[r] for r in range(top - 1)] + [last]
    z = lax.broadcasted_iota(jnp.int32, (depth, levels), 0)

    def cell(r, x, before, after):
        here = plane_of(tracer[r], x)
        spread = before + after
        if r > 0:
            spread += plane_of(tracer[r - 1], x)
        if r < top:
            spread += plane_of(tracer[r + 1], x)
        spread += jnp.where(z == 0, 0.0, pltpu.roll(here, 1, 0))
        spread += jnp.where(z == depth - 1, 0.0, pltpu.roll(here, depth - 1, 0))
        value = here + mobility[r, x] * (spread - 6.0 * here) + source[r, x]
        out[r][x] = value
        if with_stats and 0 < r < top:
            mean, squares = line_stats(value)
            stats[0][0, r - 1, pl.ds(x, 1)] = mean
            stats[0][1, r - 1, pl.ds(x, 1)] = squares

    for r in range(top + 1):
        cell(r, 0, low_x[r], plane_of(tracer[r], 1))

        @pl.loop(1, width - 1)
        def _(x, r=r):
            cell(r, x, plane_of(tracer[r], x - 1), plane_of(tracer[r], x + 1))

        cell(r, width - 1, plane_of(tracer[r], width - 2), high_x[r])


def is_even():
    return lax.rem(lax.axis_index("down"), 2) == 0


def add_lines(row, mobility, far, near, r, x):
    end, depth = (row.shape[1] - 1, mobility.shape[2])
    low_z, high_z = sides_of(far, near, r, x)
    row[x, 0:1] += mobility[r, x, 0:1] * low_z
    row[x, end : end + 1] += mobility[r, x, depth - 1 : depth] * high_z


def sides_of(far, near, r, x):
    across, beside = (far[r, pl.ds(x, 1)], near[r, pl.ds(x, 1)])
    even = is_even()
    return jnp.where(even, across, beside), jnp.where(even, beside, across)


def inner_kernel(first_in, last_in, mobility, low_y, high_y, first, last):
    top = mobility.shape[0] - 1
    rim = (mobility.shape[2] - first.shape[1]) // 2
    inside = slice(rim, mobility.shape[2] - rim)

    @pl.loop(0, first.shape[0])
    def _(x):
        first[x] = first_in[x, inside] + mobility[0, x, inside] * low_y[x]
        last[x] = last_in[x, inside] + mobility[top, x, inside] * high_y[x]


def add_outer(row_in, row, mobility, beside, r, x):
    rim, depth = (row.shape[1] // 2, mobility.shape[2])
    row[x, :rim] = row_in[x, :rim] + mobility[r, x, :rim] * beside[x, :rim]
    row[x, rim:] = row_in[x, depth - rim :] + mobility[r, x, depth - rim :] * beside[x, rim:]


def outer_kernel(first_in, last_in, mobility, low_y, high_y, far, near, first, last):
    top = mobility.shape[0] - 1

    @pl.loop(0, first.shape[0])
    def _(x):
        add_outer(first_in, first, mobility, low_y, 0, x)
        add_outer(last_in, last, mobility, high_y, top, x)
        add_lines(first, mobility, far, near, 0, x)
        add_lines(last, mobility, far, near, top, x)


def take_edges(rows, first_x, last_x, far, near):
    width = far.shape[1]
    even = is_even()
    for r, row in enumerate(rows):
        outer = row[-1]
        end = outer.shape[1] - 1

        @pl.loop(0, width)
        def _(x, r=r, outer=outer, end=end):
            leading, trailing = (outer[x, 0:1], outer[x, end : end + 1])
            far[r, pl.ds(x, 1)] = jnp.where(even, leading, trailing)
            near[r, pl.ds(x, 1)] = jnp.where(even, trailing, leading)

        first_x[r] = plane_of(row, 0)
        last_x[r] = plane_of(row, width - 1)


def edges_kernel(middle_in, *refs):
    ends, (mobility, far, near, middle), edges = (refs[:4], refs[4:8], refs[8:])

    @pl.loop(0, mobility.shape[1])
    def _(x):
        for r in range(1, mobility.shape[0] - 1):
            add_lines(middle.at[r - 1], mobility, far, near, r, x)

    take_edges(rows_of((*ends[:2], middle, *ends[2:])), *edges)


def take_inner_kernel(tracer, first, last):
    rim = (tracer.shape[2] - first.shape[1]) // 2
    inside = slice(rim, tracer.shape[2] - rim)

    @pl.loop(0, first.shape[0])
    def _(x):
        first[x] = tracer[0, x, inside]
        last[x] = tracer[tracer.shape[0] - 1, x, inside]


def take_outer_kernel(tracer, first, last, *edges):
    rim, depth = (first.shape[1] // 2, tracer.shape[2])

    @pl.loop(0, first.shape[0])
    def _(x):
        for r, row in ((0, first), (tracer.shape[0] - 1, last)):
            row[x, :rim] = tracer[r, x, :rim]
            row[x, rim:] = tracer[r, x, depth - rim :]

    take_edges(rows_of((tracer,)), *edges)


def last_kernel(first_in, middle_in, last_in, middle_stats, mobility, *refs):
    low_inner, high_inner, low_outer, high_outer, far, near, first, middle, last, stats = refs
    top = mobility.shape[0] - 1
    width, depth, _ = first_in.shape

    @pl.loop(0, width)
    def _(x):
        low_y, high_y = ((low_inner, low_outer), (high_inner, high_outer))
        for r, row_in, row, beside in ((0, first_in, first, low_y), (top, last_in, last, high_y)):
            row[x] = row_in[x] + mobility[r, x] * plane_of(beside, x)
            add_lines(row, mobility, far, near, r, x)
            stats[0, r, pl.ds(x, 1)], stats[1, r, pl.ds(x, 1)] = line_stats(row[x])
        for r in range(1, top):
            row = middle.at[r - 1]
            mean = middle_stats[0, r - 1, pl.ds(x, 1)]
            more = squares = 0.0
            for z, line in zip((0, depth - 1), sides_of(far, near, r, x)):
                old = row[x, z : z + 1]
                added = mobility[r, x, z : z + 1] * line
                row[x, z : z + 1] = old + added
                more += added
                squares += added * (2.0 * (old - mean) + added)
            shift = more * (1.0 / depth)
            stats[0, r, pl.ds(x, 1)] = mean + shift
            stats[1, r, pl.ds(x, 1)] = middle_stats[1, r - 1, pl.ds(x, 1)] + (squares - more * shift)


def store_kernel(first, middle, last, out, sems):
    top = out.shape[0] - 1
    copies = [
        pltpu.make_async_copy(first, out.at[0], sems.at[0]),
        pltpu.make_async_copy(middle, out.at[1:top], sems.at[1]),
        pltpu.make_async_copy(last, out.at[top], sems.at[2]),
    ]
    for copy in copies:
        copy.start()
    for copy in copies:
        copy.wait()


def merged(mine, other, count):
    away = mine[0] - other[0]
    return 0.5 * (mine[0] + other[0]), mine[1] + other[1] + (0.5 * count) * (away * away)


def scale_kernel(count, first, middle, last, mine, other, out, held, sems):
    copies = []
    rows = [first] + [middle.at[r] for r in range(middle.shape[0])] + [last]
    for r, row in enumerate(rows):
        mean, squares = merged((mine[0, r], mine[1, r]), (other[0, r], other[1, r]), count)
        scale = lax.rsqrt(squares * (1.0 / (2 * count)) + 0.0001)
        for x in range(row.shape[0]):
            held[r, x] = (row[x] - mean[x : x + 1]) * scale[x : x + 1]
        copies.append(pltpu.make_async_copy(held.at[r], out.at[r], sems.at[r]))
        copies[-1].start()
    for copy in copies:
        copy.wait()


def kernel_call(kernel, *out_shape, vmem_mib=16, **options):
    params = pltpu.CompilerParams(vmem_limit_bytes=vmem_mib * 1024 * 1024)
    return pl.pallas_call(kernel, out_shape=out_shape, compiler_params=params, **options)


def body(tracer, mobility, source):
    count, width, depth, levels = tracer.shape
    row, middle = (f32(width, depth, levels), f32(count - 2, width, depth, levels))
    inner, outer = (f32(width, depth - 2 * RIM, levels), f32(width, 2 * RIM, levels))
    edge_shapes = (f32(count, depth, levels),) * 2 + (f32(count, width, levels),) * 2

    peers = lax.axis_size("down")
    near = [(i, i ^ 1) for i in range(peers)]
    far = [(i, (i + (1 if i % 2 else -1)) % peers) for i in range(peers)]

    def swap(leading, last, axis):
        peers = lax.axis_size(axis)
        up = [(i, (i + 1) % peers) for i in range(peers)]
        low = lax.ppermute(last, axis, up)
        high = lax.ppermute(leading, axis, [(b, a) for a, b in up])
        return (low, high)

    def call(kernel, *out_shape, **options):
        return kernel_call(kernel, *out_shape, **options)

    inners = call(take_inner_kernel, inner, inner)(tracer)
    inners_y = swap(*inners, "south")
    first, last, *edges = call(take_outer_kernel, outer, outer, *edge_shapes)(tracer)
    pieces = (tracer,)
    outers = (first, last)
    for step in range(STEPS):
        final = step == STEPS - 1
        along_x = swap(*edges[:2], "east")
        along_z = (lax.ppermute(edges[2], "down", far), lax.ppermute(edges[3], "down", near))
        outers_y = swap(*outers, "south")
        stats = (f32(2, count - 2, width, levels),) if final else ()
        first, inside, last, *stats = call(
            functools.partial(partial_kernel, len(pieces), final), row, middle, row, *stats
        )(*pieces, mobility, source, *along_x)
        if not final:
            inners = call(inner_kernel, inner, inner)(first, last, mobility, *inners_y)
            inners_y_next = swap(*inners, "south")
            outers = call(outer_kernel, outer, outer)(first, last, mobility, *outers_y, *along_z)
            inside, *edges = call(
                edges_kernel, middle, *edge_shapes, input_output_aliases={0: 0}
            )(inside, inners[0], outers[0], inners[1], outers[1], mobility, *along_z)
            pieces = (inners[0], outers[0], inside, inners[1], outers[1])
            inners_y = inners_y_next
    *rows, mine = kernel_call(
        last_kernel, row, middle, row, f32(2, count, width, levels), input_output_aliases={1: 1}
    )(first, inside, last, *stats, mobility, *inners_y, *outers_y, *along_z)
    (stored,) = kernel_call(
        store_kernel,
        f32(count, width, depth, levels),
        out_specs=(pl.BlockSpec(memory_space=pl.ANY),),
        scratch_shapes=[pltpu.SemaphoreType.DMA((3,))],
    )(*rows)
    members = depth
    other = lax.ppermute(mine, "down", near)
    mine = jnp.stack(merged(mine, other, members))
    members *= 2
    other = lax.ppermute(mine, "down", [(i, (i + 2) % peers) for i in range(peers)])
    (standardized,) = kernel_call(
        functools.partial(scale_kernel, members),
        f32(count, width, depth, levels),
        out_specs=(pl.BlockSpec(memory_space=pl.ANY),),
        scratch_shapes=[pltpu.VMEM((count, width, depth, levels), jnp.float32), pltpu.SemaphoreType.DMA((count,))],
    )(*rows, mine, other)
    return (standardized, stored)


def solution(mesh):
    spec = P(("trial", "south"), "east", "down", None)
    return jax.shard_map(body, mesh=mesh, in_specs=(spec,) * 3, out_specs=(spec,) * 2, check_vma=False)
```

```python
import functools

import jax
import jax.numpy as jnp
from jax import lax
from jax.experimental import pallas as pl
from jax.experimental.pallas import tpu as pltpu
from jax.sharding import PartitionSpec as P


STEPS = 3
RIM = 16


def f32(*shape):
    return jax.ShapeDtypeStruct(shape, jnp.float32)


def plane_of(pieces, x):
    if len(pieces) == 1:
        return pieces[0][x]
    inner, outer = pieces
    rim = outer.shape[1] // 2
    return jnp.concatenate([outer[x, :rim], inner[x], outer[x, rim:]], axis=0)


def rows_of(refs):
    if len(refs) == 1:
        return [(refs[0].at[r],) for r in range(refs[0].shape[0])]
    half = len(refs) // 2
    middle = refs[half]
    return [refs[:half]] + [(middle.at[r],) for r in range(middle.shape[0])] + [refs[half + 1 :]]


def line_stats(value):
    mean = jnp.sum(value, axis=0, keepdims=True) * (1.0 / value.shape[0])
    off = value - mean
    return mean, jnp.sum(off * off, axis=0, keepdims=True)


def partial_kernel(n, with_stats, *refs):
    tracer = rows_of(refs[:n])
    mobility, source, low_x, high_x, first, middle, last, *stats = refs[n:]
    top, width, depth, levels = (mobility.shape[0] - 1, *mobility.shape[1:])
    out = [first] + [middle.at[r] for r in range(top - 1)] + [last]
    z = lax.broadcasted_iota(jnp.int32, (depth, levels), 0)

    def cell(r, x, before, after):
        here = plane_of(tracer[r], x)
        spread = before + after
        if r > 0:
            spread += plane_of(tracer[r - 1], x)
        if r < top:
            spread += plane_of(tracer[r + 1], x)
        spread += jnp.where(z == 0, 0.0, pltpu.roll(here, 1, 0))
        spread += jnp.where(z == depth - 1, 0.0, pltpu.roll(here, depth - 1, 0))
        value = here + mobility[r, x] * (spread - 6.0 * here) + source[r, x]
        out[r][x] = value
        if with_stats and 0 < r < top:
            mean, squares = line_stats(value)
            stats[0][0, r - 1, pl.ds(x, 1)] = mean
            stats[0][1, r - 1, pl.ds(x, 1)] = squares

    for r in range(top + 1):
        cell(r, 0, low_x[r], plane_of(tracer[r], 1))

        @pl.loop(1, width - 1)
        def _(x, r=r):
            cell(r, x, plane_of(tracer[r], x - 1), plane_of(tracer[r], x + 1))

        cell(r, width - 1, plane_of(tracer[r], width - 2), high_x[r])


def is_even():
    return lax.rem(lax.axis_index("down"), 2) == 0


def add_lines(row, mobility, far, near, r, x):
    end, depth = (row.shape[1] - 1, mobility.shape[2])
    low_z, high_z = sides_of(far, near, r, x)
    row[x, 0:1] += mobility[r, x, 0:1] * low_z
    row[x, end : end + 1] += mobility[r, x, depth - 1 : depth] * high_z


def sides_of(far, near, r, x):
    across, beside = (far[r, pl.ds(x, 1)], near[r, pl.ds(x, 1)])
    even = is_even()
    return jnp.where(even, across, beside), jnp.where(even, beside, across)


def inner_kernel(first_in, last_in, mobility, low_y, high_y, first, last, *stats):
    top = mobility.shape[0] - 1
    rim = (mobility.shape[2] - first.shape[1]) // 2
    inside = slice(rim, mobility.shape[2] - rim)

    @pl.loop(0, first.shape[0])
    def _(x):
        ends = ((0, first_in, first, low_y), (top, last_in, last, high_y))
        for i, (r, row_in, row, beside) in enumerate(ends):
            value = row_in[x, inside] + mobility[r, x, inside] * beside[x]
            row[x] = value
            for part in stats:
                part[0, i, pl.ds(x, 1)], part[1, i, pl.ds(x, 1)] = line_stats(value)


def add_outer(row_in, row, mobility, beside, r, x):
    rim, depth = (row.shape[1] // 2, mobility.shape[2])
    row[x, :rim] = row_in[x, :rim] + mobility[r, x, :rim] * beside[x, :rim]
    row[x, rim:] = row_in[x, depth - rim :] + mobility[r, x, depth - rim :] * beside[x, rim:]


def outer_kernel(first_in, last_in, mobility, low_y, high_y, far, near, first, last):
    top = mobility.shape[0] - 1

    @pl.loop(0, first.shape[0])
    def _(x):
        add_outer(first_in, first, mobility, low_y, 0, x)
        add_outer(last_in, last, mobility, high_y, top, x)
        add_lines(first, mobility, far, near, 0, x)
        add_lines(last, mobility, far, near, top, x)


def take_edges(rows, first_x, last_x, far, near):
    width = far.shape[1]
    even = is_even()
    for r, row in enumerate(rows):
        outer = row[-1]
        end = outer.shape[1] - 1

        @pl.loop(0, width)
        def _(x, r=r, outer=outer, end=end):
            leading, trailing = (outer[x, 0:1], outer[x, end : end + 1])
            far[r, pl.ds(x, 1)] = jnp.where(even, leading, trailing)
            near[r, pl.ds(x, 1)] = jnp.where(even, trailing, leading)

        first_x[r] = plane_of(row, 0)
        last_x[r] = plane_of(row, width - 1)


def edges_kernel(middle_in, *refs):
    ends, (mobility, far, near, middle), edges = (refs[:4], refs[4:8], refs[8:])

    @pl.loop(0, mobility.shape[1])
    def _(x):
        for r in range(1, mobility.shape[0] - 1):
            add_lines(middle.at[r - 1], mobility, far, near, r, x)

    take_edges(rows_of((*ends[:2], middle, *ends[2:])), *edges)


def take_outer_kernel(tracer, first, last, *edges):
    rim, depth = (first.shape[1] // 2, tracer.shape[2])

    @pl.loop(0, first.shape[0])
    def _(x):
        for r, row in ((0, first), (tracer.shape[0] - 1, last)):
            row[x, :rim] = tracer[r, x, :rim]
            row[x, rim:] = tracer[r, x, depth - rim :]

    take_edges(rows_of((tracer,)), *edges)


def joined(one, other, count, other_count):
    away, share = (other[0] - one[0], other_count / (count + other_count))
    return one[0] + share * away, one[1] + other[1] + (count * share) * (away * away)


def middle_kernel(middle_in, stats_in, mobility, far, near, middle, stats):
    width, depth = mobility.shape[1:3]

    @pl.loop(0, width)
    def _(x):
        for r in range(1, mobility.shape[0] - 1):
            row = middle.at[r - 1]
            mean = stats_in[0, r - 1, pl.ds(x, 1)]
            more = squares = 0.0
            for z, line in zip((0, depth - 1), sides_of(far, near, r, x)):
                old = row[x, z : z + 1]
                added = mobility[r, x, z : z + 1] * line
                row[x, z : z + 1] = old + added
                more += added
                squares += added * (2.0 * (old - mean) + added)
            shift = more * (1.0 / depth)
            stats[0, r - 1, pl.ds(x, 1)] = mean + shift
            stats[1, r - 1, pl.ds(x, 1)] = stats_in[1, r - 1, pl.ds(x, 1)] + (squares - more * shift)


def last_kernel(first_in, last_in, inner_stats, mobility, *refs):
    low_outer, high_outer, far, near, first, last, stats = refs
    top = mobility.shape[0] - 1
    width, depth, _ = first_in.shape
    count = first.shape[1]

    @pl.loop(0, width, unroll=8)
    def _(x):
        ends = ((0, first_in, first, low_outer), (top, last_in, last, high_outer))
        for i, (r, row_in, row, beside) in enumerate(ends):
            add_outer(row_in, row, mobility, beside, r, x)
            add_lines(row, mobility, far, near, r, x)
            inner = (inner_stats[0, i, pl.ds(x, 1)], inner_stats[1, i, pl.ds(x, 1)])
            stats[0, i, pl.ds(x, 1)], stats[1, i, pl.ds(x, 1)] = joined(
                inner, line_stats(row[x]), depth - count, count
            )


def store_kernel(first_inner, first_outer, middle, last_inner, last_outer, out, sems):
    top, depth, rim = (out.shape[0] - 1, out.shape[2], first_outer.shape[1] // 2)
    pairs = [(middle, out.at[pl.ds(1, top - 1)])]
    for r, inner, outer in ((0, first_inner, first_outer), (top, last_inner, last_outer)):
        pairs.append((inner, out.at[r, :, pl.ds(rim, depth - 2 * rim)]))
        pairs.append((outer.at[:, pl.ds(0, rim)], out.at[r, :, pl.ds(0, rim)]))
        pairs.append((outer.at[:, pl.ds(rim, rim)], out.at[r, :, pl.ds(depth - rim, rim)]))
    copies = [pltpu.make_async_copy(*pair, sems.at[i]) for i, pair in enumerate(pairs)]
    for copy in copies:
        copy.start()
    for copy in copies:
        copy.wait()


def scale_kernel(count, *refs):
    *rows, mine, other, out, held, sems = refs
    width = held.shape[1]
    share = width * held.shape[0] // sems.shape[0]
    copies = []
    for r, row in enumerate(rows_of(rows)):
        mean, squares = joined((mine[0, r], mine[1, r]), (other[0, r], other[1, r]), count, count)
        scale = lax.rsqrt(squares * (1.0 / (2 * count)) + 0.0001)
        for x in range(width):
            held[r, x] = (plane_of(row, x) - mean[x : x + 1]) * scale[x : x + 1]
            if (x + 1) % share == 0:
                planes = pl.ds(x + 1 - share, share)
                copies.append(pltpu.make_async_copy(held.at[r, planes], out.at[r, planes], sems.at[len(copies)]))
                copies[-1].start()
    for copy in copies:
        copy.wait()


def kernel_call(kernel, *out_shape, vmem_mib=16, **options):
    params = pltpu.CompilerParams(vmem_limit_bytes=vmem_mib * 1024 * 1024)
    return pl.pallas_call(kernel, out_shape=out_shape, compiler_params=params, **options)


def body(tracer, mobility, source):
    count, width, depth, levels = tracer.shape
    row, middle = (f32(width, depth, levels), f32(count - 2, width, depth, levels))
    inner, outer = (f32(width, depth - 2 * RIM, levels), f32(width, 2 * RIM, levels))
    edge_shapes = (f32(count, depth, levels),) * 2 + (f32(count, width, levels),) * 2

    peers = lax.axis_size("down")
    near = [(i, i ^ 1) for i in range(peers)]
    far = [(i, (i + (1 if i % 2 else -1)) % peers) for i in range(peers)]

    def swap(leading, last, axis):
        peers = lax.axis_size(axis)
        up = [(i, (i + 1) % peers) for i in range(peers)]
        low = lax.ppermute(last, axis, up)
        high = lax.ppermute(leading, axis, [(b, a) for a, b in up])
        return (low, high)

    def call(kernel, *out_shape, **options):
        return kernel_call(kernel, *out_shape, **options)

    inners = (tracer[0, :, RIM : depth - RIM], tracer[-1, :, RIM : depth - RIM])
    inners_y = swap(*inners, "south")
    first, last, *edges = call(take_outer_kernel, outer, outer, *edge_shapes)(tracer)
    pieces = (tracer,)
    outers = (first, last)
    for step in range(STEPS):
        final = step == STEPS - 1
        along_x = swap(*edges[:2], "east")
        along_z = (lax.ppermute(edges[2], "down", far), lax.ppermute(edges[3], "down", near))
        outers_y = swap(*outers, "south")
        stats = (f32(2, count - 2, width, levels),) if final else ()
        first, inside, last, *stats = call(
            functools.partial(partial_kernel, len(pieces), final), row, middle, row, *stats
        )(*pieces, mobility, source, *along_x)
        end_stats = (f32(2, 2, width, levels),) if final else ()
        *inners, end_stats = (
            *call(inner_kernel, inner, inner, *end_stats)(first, last, mobility, *inners_y),
            *(() if final else (None,)),
        )
        if not final:
            inners_y_next = swap(*inners, "south")
            outers = call(outer_kernel, outer, outer)(first, last, mobility, *outers_y, *along_z)
            inside, *edges = call(
                edges_kernel, middle, *edge_shapes, input_output_aliases={0: 0}
            )(inside, inners[0], outers[0], inners[1], outers[1], mobility, *along_z)
            pieces = (inners[0], outers[0], inside, inners[1], outers[1])
            inners_y = inners_y_next
    inside, middle_stats = call(
        middle_kernel, middle, f32(2, count - 2, width, levels), input_output_aliases={0: 0}
    )(inside, *stats, mobility, *along_z)
    *outers, mine = call(last_kernel, outer, outer, f32(2, 2, width, levels))(
        first, last, end_stats, mobility, *outers_y, *along_z
    )
    mine = jnp.concatenate([mine[:, :1], middle_stats, mine[:, 1:]], axis=1)
    rows = (inners[0], outers[0], inside, inners[1], outers[1])
    (stored,) = call(
        store_kernel,
        f32(count, width, depth, levels),
        out_specs=(pl.BlockSpec(memory_space=pl.ANY),),
        scratch_shapes=[pltpu.SemaphoreType.DMA((7,))],
    )(*rows)
    members = depth
    other = lax.ppermute(mine, "down", near)
    mine = jnp.stack(joined(mine, other, members, members))
    members *= 2
    other = lax.ppermute(mine, "down", [(i, (i + 2) % peers) for i in range(peers)])
    (standardized,) = call(
        functools.partial(scale_kernel, members),
        f32(count, width, depth, levels),
        out_specs=(pl.BlockSpec(memory_space=pl.ANY),),
        scratch_shapes=[pltpu.VMEM((count, width, depth, levels), jnp.float32), pltpu.SemaphoreType.DMA((2 * count,))],
    )(*rows, mine, other)
    return (standardized, stored)


def solution(mesh):
    spec = P(("trial", "south"), "east", "down", None)
    return jax.shard_map(body, mesh=mesh, in_specs=(spec,) * 3, out_specs=(spec,) * 2, check_vma=False)
```

```python
import functools

import jax
import jax.numpy as jnp
from jax import lax
from jax.experimental import pallas as pl
from jax.experimental.pallas import tpu as pltpu
from jax.sharding import PartitionSpec as P


STEPS = 3
RIM = 16


def f32(*shape):
    return jax.ShapeDtypeStruct(shape, jnp.float32)


def plane_of(pieces, x):
    if len(pieces) == 1:
        return pieces[0][x]
    inner, outer = pieces
    rim = outer.shape[1] // 2
    return jnp.concatenate([outer[x, :rim], inner[x], outer[x, rim:]], axis=0)


def rows_of(refs):
    if len(refs) == 1:
        return [(refs[0].at[r],) for r in range(refs[0].shape[0])]
    half = len(refs) // 2
    middle = refs[half]
    return [refs[:half]] + [(middle.at[r],) for r in range(middle.shape[0])] + [refs[half + 1 :]]


def line_stats(value):
    mean = jnp.sum(value, axis=0, keepdims=True) * (1.0 / value.shape[0])
    off = value - mean
    return mean, jnp.sum(off * off, axis=0, keepdims=True)


def partial_kernel(n, with_stats, *refs):
    tracer = rows_of(refs[:n])
    mobility, source, low_x, high_x, first, middle, last, *stats = refs[n:]
    top, width, depth, levels = (mobility.shape[0] - 1, *mobility.shape[1:])
    out = [first] + [middle.at[r] for r in range(top - 1)] + [last]
    z = lax.broadcasted_iota(jnp.int32, (depth, levels), 0)

    def cell(r, x, before, after):
        here = plane_of(tracer[r], x)
        spread = before + after
        if r > 0:
            spread += plane_of(tracer[r - 1], x)
        if r < top:
            spread += plane_of(tracer[r + 1], x)
        spread += jnp.where(z == 0, 0.0, pltpu.roll(here, 1, 0))
        spread += jnp.where(z == depth - 1, 0.0, pltpu.roll(here, depth - 1, 0))
        value = here + mobility[r, x] * (spread - 6.0 * here) + source[r, x]
        out[r][x] = value
        if with_stats and 0 < r < top:
            mean, squares = line_stats(value)
            stats[0][0, r - 1, pl.ds(x, 1)] = mean
            stats[0][1, r - 1, pl.ds(x, 1)] = squares

    for r in range(top + 1):
        cell(r, 0, low_x[r], plane_of(tracer[r], 1))

        @pl.loop(1, width - 1)
        def _(x, r=r):
            cell(r, x, plane_of(tracer[r], x - 1), plane_of(tracer[r], x + 1))

        cell(r, width - 1, plane_of(tracer[r], width - 2), high_x[r])


def is_even():
    return lax.rem(lax.axis_index("down"), 2) == 0


def add_lines(row, mobility, far, near, r, x):
    end, depth = (row.shape[1] - 1, mobility.shape[2])
    low_z, high_z = sides_of(far, near, r, x)
    row[x, 0:1] += mobility[r, x, 0:1] * low_z
    row[x, end : end + 1] += mobility[r, x, depth - 1 : depth] * high_z


def sides_of(far, near, r, x):
    across, beside = (far[r, pl.ds(x, 1)], near[r, pl.ds(x, 1)])
    even = is_even()
    return jnp.where(even, across, beside), jnp.where(even, beside, across)


def inner_kernel(first_in, last_in, mobility, low_y, high_y, first, last, *stats):
    top = mobility.shape[0] - 1
    rim = (mobility.shape[2] - first.shape[1]) // 2
    inside = slice(rim, mobility.shape[2] - rim)

    @pl.loop(0, first.shape[0])
    def _(x):
        ends = ((0, first_in, first, low_y), (top, last_in, last, high_y))
        for i, (r, row_in, row, beside) in enumerate(ends):
            value = row_in[x, inside] + mobility[r, x, inside] * beside[x]
            row[x] = value
            for part in stats:
                part[0, i, pl.ds(x, 1)], part[1, i, pl.ds(x, 1)] = line_stats(value)


def add_outer(row_in, row, mobility, beside, r, x):
    rim, depth = (row.shape[1] // 2, mobility.shape[2])
    row[x, :rim] = row_in[x, :rim] + mobility[r, x, :rim] * beside[x, :rim]
    row[x, rim:] = row_in[x, depth - rim :] + mobility[r, x, depth - rim :] * beside[x, rim:]


def outer_kernel(first_in, last_in, mobility, low_y, high_y, far, near, first, last):
    top = mobility.shape[0] - 1

    @pl.loop(0, first.shape[0])
    def _(x):
        add_outer(first_in, first, mobility, low_y, 0, x)
        add_outer(last_in, last, mobility, high_y, top, x)
        add_lines(first, mobility, far, near, 0, x)
        add_lines(last, mobility, far, near, top, x)


def take_edges(rows, first_x, last_x, far, near):
    width = far.shape[1]
    even = is_even()
    for r, row in enumerate(rows):
        outer = row[-1]
        end = outer.shape[1] - 1

        @pl.loop(0, width)
        def _(x, r=r, outer=outer, end=end):
            leading, trailing = (outer[x, 0:1], outer[x, end : end + 1])
            far[r, pl.ds(x, 1)] = jnp.where(even, leading, trailing)
            near[r, pl.ds(x, 1)] = jnp.where(even, trailing, leading)

        first_x[r] = plane_of(row, 0)
        last_x[r] = plane_of(row, width - 1)


def edges_kernel(middle_in, *refs):
    ends, (mobility, far, near, middle), edges = (refs[:4], refs[4:8], refs[8:])

    @pl.loop(0, mobility.shape[1])
    def _(x):
        for r in range(1, mobility.shape[0] - 1):
            add_lines(middle.at[r - 1], mobility, far, near, r, x)

    take_edges(rows_of((*ends[:2], middle, *ends[2:])), *edges)


def take_outer_kernel(tracer, first, last, *edges):
    rim, depth = (first.shape[1] // 2, tracer.shape[2])

    @pl.loop(0, first.shape[0])
    def _(x):
        for r, row in ((0, first), (tracer.shape[0] - 1, last)):
            row[x, :rim] = tracer[r, x, :rim]
            row[x, rim:] = tracer[r, x, depth - rim :]

    take_edges(rows_of((tracer,)), *edges)


def joined(one, other, count, other_count):
    away, share = (other[0] - one[0], other_count / (count + other_count))
    return one[0] + share * away, one[1] + other[1] + (count * share) * (away * away)


def middle_kernel(middle_in, stats_in, mobility, far, near, middle, stats):
    width, depth = mobility.shape[1:3]

    @pl.loop(0, width)
    def _(x):
        for r in range(1, mobility.shape[0] - 1):
            row = middle.at[r - 1]
            mean = stats_in[0, r - 1, pl.ds(x, 1)]
            more = squares = 0.0
            for z, line in zip((0, depth - 1), sides_of(far, near, r, x)):
                old = row[x, z : z + 1]
                added = mobility[r, x, z : z + 1] * line
                row[x, z : z + 1] = old + added
                more += added
                squares += added * (2.0 * (old - mean) + added)
            shift = more * (1.0 / depth)
            stats[0, r - 1, pl.ds(x, 1)] = mean + shift
            stats[1, r - 1, pl.ds(x, 1)] = stats_in[1, r - 1, pl.ds(x, 1)] + (squares - more * shift)


def last_kernel(first_in, last_in, inner_stats, mobility, *refs):
    low_outer, high_outer, far, near, first, last, stats = refs
    top = mobility.shape[0] - 1
    width, depth, _ = first_in.shape
    count = first.shape[1]

    @pl.loop(0, width, unroll=8)
    def _(x):
        ends = ((0, first_in, first, low_outer), (top, last_in, last, high_outer))
        for i, (r, row_in, row, beside) in enumerate(ends):
            add_outer(row_in, row, mobility, beside, r, x)
            add_lines(row, mobility, far, near, r, x)
            inner = (inner_stats[0, i, pl.ds(x, 1)], inner_stats[1, i, pl.ds(x, 1)])
            stats[0, i, pl.ds(x, 1)], stats[1, i, pl.ds(x, 1)] = joined(
                inner, line_stats(row[x]), depth - count, count
            )


def store_kernel(first_inner, first_outer, middle, last_inner, last_outer, out, sems):
    top, depth, rim = (out.shape[0] - 1, out.shape[2], first_outer.shape[1] // 2)
    pairs = [(middle, out.at[pl.ds(1, top - 1)])]
    for r, inner, outer in ((0, first_inner, first_outer), (top, last_inner, last_outer)):
        pairs.append((inner, out.at[r, :, pl.ds(rim, depth - 2 * rim)]))
        pairs.append((outer.at[:, pl.ds(0, rim)], out.at[r, :, pl.ds(0, rim)]))
        pairs.append((outer.at[:, pl.ds(rim, rim)], out.at[r, :, pl.ds(depth - rim, rim)]))
    copies = [pltpu.make_async_copy(*pair, sems.at[i]) for i, pair in enumerate(pairs)]
    for copy in copies:
        copy.start()
    for copy in copies:
        copy.wait()


def scale_kernel(count, *refs):
    *rows, mine, other, out, held, sems = refs
    width = held.shape[1]
    share = width * held.shape[0] // sems.shape[0]
    copies = []
    for r, row in enumerate(rows_of(rows)):
        mean, squares = joined((mine[0, r], mine[1, r]), (other[0, r], other[1, r]), count, count)
        scale = lax.rsqrt(squares * (1.0 / (2 * count)) + 0.0001)
        for x in range(width):
            held[r, x] = (plane_of(row, x) - mean[x : x + 1]) * scale[x : x + 1]
            if (x + 1) % share == 0:
                planes = pl.ds(x + 1 - share, share)
                copies.append(pltpu.make_async_copy(held.at[r, planes], out.at[r, planes], sems.at[len(copies)]))
                copies[-1].start()
    for copy in copies:
        copy.wait()


def kernel_call(kernel, *out_shape, vmem_mib=16, **options):
    params = pltpu.CompilerParams(vmem_limit_bytes=vmem_mib * 1024 * 1024)
    return pl.pallas_call(kernel, out_shape=out_shape, compiler_params=params, **options)


def body(tracer, mobility, source):
    count, width, depth, levels = tracer.shape
    row, middle = (f32(width, depth, levels), f32(count - 2, width, depth, levels))
    inner, outer = (f32(width, depth - 2 * RIM, levels), f32(width, 2 * RIM, levels))
    edge_shapes = (f32(count, depth, levels),) * 2 + (f32(count, width, levels),) * 2

    peers = lax.axis_size("down")
    near = [(i, i ^ 1) for i in range(peers)]
    far = [(i, (i + (1 if i % 2 else -1)) % peers) for i in range(peers)]

    def sent(value, axis, pairs):
        return lax.ppermute(value, axis, pairs)

    def swap(leading, last, axis):
        peers = lax.axis_size(axis)
        up = [(i, (i + 1) % peers) for i in range(peers)]
        low = sent(last, axis, up)
        high = sent(leading, axis, [(b, a) for a, b in up])
        return (low, high)

    def call(kernel, *out_shape, **options):
        return kernel_call(kernel, *out_shape, **options)

    inners = (tracer[0, :, RIM : depth - RIM], tracer[-1, :, RIM : depth - RIM])
    inners_y = swap(*inners, "south")
    first, last, *edges = call(take_outer_kernel, outer, outer, *edge_shapes)(tracer)
    pieces = (tracer,)
    outers = (first, last)
    for step in range(STEPS):
        final = step == STEPS - 1
        along_x = swap(*edges[:2], "east")
        along_z = (sent(edges[2], "down", far), sent(edges[3], "down", near))
        outers_y = swap(*outers, "south")
        stats = (f32(2, count - 2, width, levels),) if final else ()
        first, inside, last, *stats = call(
            functools.partial(partial_kernel, len(pieces), final), row, middle, row, *stats
        )(*pieces, mobility, source, *along_x)
        end_stats = (f32(2, 2, width, levels),) if final else ()
        *inners, end_stats = (
            *call(inner_kernel, inner, inner, *end_stats)(first, last, mobility, *inners_y),
            *(() if final else (None,)),
        )
        if not final:
            inners_y_next = swap(*inners, "south")
            outers = call(outer_kernel, outer, outer)(first, last, mobility, *outers_y, *along_z)
            inside, *edges = call(
                edges_kernel, middle, *edge_shapes, input_output_aliases={0: 0}
            )(inside, inners[0], outers[0], inners[1], outers[1], mobility, *along_z)
            pieces = (inners[0], outers[0], inside, inners[1], outers[1])
            inners_y = inners_y_next
    inside, middle_stats = call(
        middle_kernel, middle, f32(2, count - 2, width, levels), input_output_aliases={0: 0}
    )(inside, *stats, mobility, *along_z)
    *outers, mine = call(last_kernel, outer, outer, f32(2, 2, width, levels))(
        first, last, end_stats, mobility, *outers_y, *along_z
    )
    rows = (inners[0], outers[0], inside, inners[1], outers[1])
    (stored,) = call(
        store_kernel,
        f32(count, width, depth, levels),
        out_specs=(pl.BlockSpec(memory_space=pl.ANY),),
        scratch_shapes=[pltpu.SemaphoreType.DMA((7,))],
    )(*rows)
    members = depth
    pairs = (middle_stats, mine)
    middle_stats, mine = (
        jnp.stack(joined(stats, sent(stats, "down", near), members, members)) for stats in pairs
    )
    mine = jnp.concatenate([mine[:, :1], middle_stats, mine[:, 1:]], axis=1)
    members *= 2
    other = sent(mine, "down", [(i, (i + 2) % peers) for i in range(peers)])
    (standardized,) = call(
        functools.partial(scale_kernel, members),
        f32(count, width, depth, levels),
        out_specs=(pl.BlockSpec(memory_space=pl.ANY),),
        scratch_shapes=[pltpu.VMEM((count, width, depth, levels), jnp.float32), pltpu.SemaphoreType.DMA((2 * count,))],
    )(*rows, mine, other)
    return (standardized, stored)


def solution(mesh):
    spec = P(("trial", "south"), "east", "down", None)
    return jax.shard_map(body, mesh=mesh, in_specs=(spec,) * 3, out_specs=(spec,) * 2, check_vma=False)
```
